32 devices in a mesh: dp: 8 (over y, x, core), seq: 4 (over z).
Axes of the slice: x: 2, y: 2, z: 4, core: 2. Of those that a mesh axis runs over, the one named last changes fastest.
Arguments:
- student_in: bfloat16 [4096, 3584], P(('dp', 'seq')), may hold values from -6 to 6
- weight: bfloat16 [3584, 512], P(('dp', 'seq')), may hold values from -0.09375 to 0.09375
- queries: bfloat16 [4096, 512], P(('dp', 'seq')), may hold values from -8 to 8, as said below
- keys: bfloat16 [4096, 128], P(('dp', 'seq')), may hold values from -8 to 8
- values: bfloat16 [4096, 128], P(('dp', 'seq')), may hold values from -6 to 6
- lengths: int32 [8, 4], P('dp'), may hold values from 1 to 384, 512 in all within a row
- assignment: int32 [8, 4], P('dp'), may hold values from 0 to 3, each once within a row
Outputs:
- attention: bfloat16 [4096, 512], P(('dp', 'seq'))
- weight_grad: float32 [3584, 512], P(('dp', 'seq'))
The draws below stay inside these ranges and needn't reach their ends.
Inputs may be any that keep to these rules, and one draw needn't show every extreme that they name: `queries`: entries of head 0 and of keys may reach the ends of this range. Each row holds the lengths of 4 rollouts of one sequence, summing to 512, the longest exactly 384. `assignment`: each row is a permutation of the 4 rollout blocks of one sequence.
All inputs are finite; a program needn't handle non-finite values.
Results may differ from the reference program's by a relative error of at most 0.012.
Values may be sent and summed in bfloat16 or wider, within the bound.
A program may use at most 64 MiB of HBM per device.

```python
import math
import jax
import jax.numpy as jnp
import numpy as np
from jax import lax

HD = 128
HQ = 4
DS = 3584
BLK = 128
DOCS = 4
SEQLEN = 512
TOKENS_ALL = 4096
NBLK = 4
MAXLEN = 384
N_DP = 8


def draw_queries(key, part):
    noise_key = jax.random.fold_in(key, 11)
    drawn = jnp.clip(jax.random.normal(noise_key, (TOKENS_ALL, HQ * HD), jnp.float32), -8.0, 8.0)
    return drawn.astype(jnp.bfloat16)


def draw_keys(key, part):
    noise_key = jax.random.fold_in(key, 13)
    drawn = jnp.clip(jax.random.normal(noise_key, (TOKENS_ALL, HD), jnp.float32), -8.0, 8.0)
    return drawn.astype(jnp.bfloat16)


def with_spikes(values, key, source, target, blocks, factor):
    def block_of(axis_at):
        return (jnp.arange(values.shape[axis_at]) // (values.shape[axis_at] // blocks)).reshape((-1,) + (1,) * (values.ndim - 1 - axis_at))

    first = jax.random.permutation(key, blocks)[block_of(target)]
    far = (block_of(target) + blocks // 2) % blocks
    return jnp.where((block_of(source) == first) | (block_of(source) == far), factor * values, values)


def block_scale(rng, dims, split, least, largest):
    gain = 1.0
    for dim, blocks in split:
        steps = jax.random.uniform(jax.random.fold_in(jax.random.fold_in(rng, 6), dim), (blocks,), jnp.float32, least / len(split), largest / len(split))
        gain = gain * jnp.repeat(jnp.exp(steps), dims[dim] // blocks).reshape((-1,) + (1,) * (len(dims) - 1 - dim))
    return gain


def split_up(amount, total, limit, lean):
    weights = [(1 << 20) // math.isqrt(grade ** lean) + 1 for grade in range(2, amount + 1)]
    rest, holding = total - limit - (amount - 1), [1] * (amount - 1)
    while rest > 0:
        candidates = [i for i in range(amount - 1) if holding[i] < limit]
        mass, left = sum([weights[i] for i in candidates]), rest
        for i in candidates:
            extra = min(limit - holding[i], max(1, left * weights[i] // mass), rest)
            holding[i] = holding[i] + extra
            rest = rest - extra
    return np.array([limit] + holding)


def uneven_parts(own_key, count, total, bound, lean):
    if count == 2:
        one = jax.random.randint(own_key, (), max(1, total - bound), min(bound, total - 1) + 1)
        return jnp.stack([one, total - one])
    sizes = jnp.asarray(split_up(count, total, bound, lean), jnp.int32)
    pairs = (count - 1) // 2
    donor, taker = sizes[1:1 + 2 * pairs:2], sizes[2:2 + 2 * pairs:2]
    slack = jnp.minimum(donor - 1, bound - taker)
    moved = jax.random.randint(jax.random.fold_in(own_key, 1), (pairs,), 0, 1 << 20) % (slack + 1)
    sizes = sizes.at[1:1 + 2 * pairs:2].set(donor - moved).at[2:2 + 2 * pairs:2].set(taker + moved)
    return sizes[jax.random.permutation(jax.random.fold_in(own_key, 2), count)]


def scatter_about(own_key, extent, scale, reach, cuts=(), kind=jnp.bfloat16):
    result = scale * jax.random.normal(own_key, extent, jnp.float32)
    if cuts:
        result = result * block_scale(own_key, extent, cuts, -0.22, 0.18)
    return jnp.clip(result, -reach, reach).astype(kind)


def bell_draw_with(own_key, shape, width, most, shards, heavy, kind=jnp.bfloat16):
    values = width * jax.random.normal(own_key, shape, jnp.float32)
    if shards:
        values = values * block_scale(own_key, shape, shards, -0.22, 0.18)
    return jnp.clip(with_spikes(values, jax.random.fold_in(own_key, 3), *heavy), -most, most).astype(kind)


def setup_inputs(seed: int = 0) -> dict:
    arg_keys = jax.random.split(jax.random.key(seed), 8)
    student_in = bell_draw_with(arg_keys[0], (TOKENS_ALL, DS), 1.0, 6.0, ((0, 32),), (0, 1, 32, 2.75))
    weight = scatter_about(arg_keys[1], (DS, HQ * HD), DS ** -0.5, 0.09375, ((0, 32),))
    queries = draw_queries(jax.random.fold_in(arg_keys[7], 71), 0)
    keys = draw_keys(jax.random.fold_in(arg_keys[7], 71), 0)
    values = scatter_about(arg_keys[4], (TOKENS_ALL, HD), 1.0, 6.0, ((0, 32),))
    lengths = jax.vmap(lambda own: uneven_parts(own, DOCS, SEQLEN, MAXLEN, 2))(jax.random.split(arg_keys[5], N_DP)).reshape((N_DP, DOCS)).astype(jnp.int32)
    assignment = jax.vmap(lambda own: jax.random.permutation(own, NBLK))(jax.random.split(arg_keys[6], N_DP)).reshape((N_DP, NBLK)).astype(jnp.int32)
    return {"student_in": student_in, "weight": weight, "queries": queries, "keys": keys, "values": values, "lengths": lengths, "assignment": assignment}


EPSILON = 1e-06
NEGATIVE = -1e+30

def locate(assign_row, length_row):
    slot_ids = jnp.arange(SEQLEN, dtype=jnp.int32)
    position = (assign_row[slot_ids // BLK] * BLK + slot_ids % BLK).astype(jnp.int32)
    doc_ends = jnp.cumsum(length_row).astype(jnp.int32)
    document = lax.optimization_barrier(jnp.sum((position[:, None] >= doc_ends[None, :]).astype(jnp.int32), axis=1))
    return (position, document)

def attend(query_rows, key_rows, value_rows, position, document):
    step_rows = math.gcd(SEQLEN, 512)
    blocks = query_rows.reshape(SEQLEN // step_rows, step_rows, HQ, HD)

    def one_block(block_items):
        query_block, query_pos, query_doc = block_items
        scores = jnp.einsum('qhd,kd->hqk', query_block.astype(jnp.float32), key_rows.astype(jnp.float32)) * HD ** (-0.5)
        allowed = (query_doc[:, None] == document[None, :]) & (query_pos[:, None] >= position[None, :])
        masked = jnp.where(allowed[None], scores, NEGATIVE)
        row_top = lax.optimization_barrier(jnp.max(masked, axis=-1, keepdims=True))
        exp_terms = jnp.where(allowed[None], jnp.exp(masked - row_top), 0.0)
        totals = lax.optimization_barrier(jnp.sum(exp_terms, axis=-1))
        rounded = lax.optimization_barrier(exp_terms.astype(jnp.bfloat16)).astype(jnp.float32)
        mixture = jnp.einsum('hqk,kd->qhd', rounded, value_rows.astype(jnp.float32))
        return (mixture / totals.T[:, :, None]).astype(jnp.bfloat16)
    attended = lax.map(one_block, (blocks, position.reshape(-1, step_rows), document.reshape(-1, step_rows)))
    return attended.reshape(SEQLEN, HQ * HD)

def reference(student_in, weight, queries, keys, values, lengths, assignment):

    def sequence(running, per_seq):
        rows_in, query_rows, key_rows, value_rows, length_row, assign_row = per_seq
        position, document = locate(assign_row, length_row)
        attended = attend(query_rows, key_rows, value_rows, position, document)
        as_float = rows_in.astype(jnp.float32)
        normed = (as_float * lax.rsqrt(lax.optimization_barrier(jnp.mean(as_float * as_float, axis=1, keepdims=True)) + EPSILON)).astype(jnp.bfloat16)
        predicted = jnp.dot(normed, weight, preferred_element_type=jnp.float32)
        scaled = ((predicted - attended.astype(jnp.float32)) * TOKENS_ALL ** (-0.5)).astype(jnp.bfloat16)
        partial_sum = lax.dot_general(normed, scaled, (((0,), (0,)), ((), ())), preferred_element_type=jnp.float32)
        return (running + partial_sum, attended)
    stacked = (student_in.reshape(N_DP, SEQLEN, DS), queries.reshape(N_DP, SEQLEN, HQ * HD), keys.reshape(N_DP, SEQLEN, HD), values.reshape(N_DP, SEQLEN, HD), lengths, assignment)
    weight_grad, attention = lax.scan(sequence, jnp.zeros((DS, HQ * HD), jnp.float32), stacked)
    return (attention.reshape(TOKENS_ALL, HQ * HD), weight_grad)
```

```python
import functools
import math

import jax
import jax.numpy as jnp
from jax import lax
from jax.experimental import pallas as pl
from jax.experimental.pallas import tpu as pltpu
from jax.sharding import PartitionSpec as P

HD = 128
HQ = 4
BLK = 128


EPSILON = 1e-06
NEGATIVE = -1e30


def locate(assign_row, doc_ends, first_slot, count):
    slot_ids = first_slot + jnp.arange(count, dtype=jnp.int32)
    block_ids = slot_ids // BLK
    block_table = jnp.arange(assign_row.shape[0], dtype=jnp.int32)
    placed = jnp.sum(
        jnp.where(block_ids[:, None] == block_table[None, :], assign_row[None, :], 0), axis=1
    )
    position = placed * BLK + slot_ids % BLK
    document = jnp.sum((position[:, None] >= doc_ends[None, :]).astype(jnp.int32), axis=1)
    return (position, document)


def absorb_block(state, key_block, value_block, query_heads, allowed):
    run_max, run_total, run_acc = state
    scores = jnp.einsum(
        "qhd,kd->hqk", query_heads, key_block, preferred_element_type=jnp.float32
    ) * HD ** (-0.5)
    masked = jnp.where(allowed[None], scores, NEGATIVE)
    new_max = jnp.maximum(run_max, jnp.max(masked, axis=-1))
    fading = jnp.exp(run_max - new_max)
    exp_terms = jnp.where(allowed[None], jnp.exp(masked - new_max[:, :, None]), 0.0)
    new_total = run_total * fading + jnp.sum(exp_terms, axis=-1)
    mixture = jnp.einsum(
        "hqk,kd->qhd",
        exp_terms.astype(jnp.bfloat16),
        value_block,
        preferred_element_type=jnp.float32,
    )
    new_acc = run_acc * fading.T[:, :, None] + mixture
    return (new_max, new_total, new_acc)


def local(student_in, weight, queries, keys, values, lengths, assignment):
    rows = queries.shape[0]
    assign_row = assignment[0]
    doc_ends = jnp.cumsum(lengths[0])
    query_pos, query_doc = locate(assign_row, doc_ends, lax.axis_index("seq") * rows, rows)
    query_heads = queries.reshape(rows, HQ, HD)
    start_state = (
        jnp.full((HQ, rows), NEGATIVE, jnp.float32),
        jnp.zeros((HQ, rows), jnp.float32),
        jnp.zeros((rows, HQ, HD), jnp.float32),
    )
    key_piece = lax.all_gather(keys, "seq", axis=0, tiled=True)
    value_piece = lax.all_gather(values, "seq", axis=0, tiled=True)
    count = key_piece.shape[0]
    step_rows = math.gcd(count, 512)
    steps_count = count // step_rows
    key_pos, key_doc = locate(assign_row, doc_ends, jnp.int32(0), count)

    def one_step(running, slabs):
        key_block, value_block, key_position, key_document = slabs
        allowed = (query_doc[:, None] == key_document[None, :]) & (
            query_pos[:, None] >= key_position[None, :]
        )
        updated = absorb_block(running, key_block, value_block, query_heads, allowed)
        return (updated, None)

    slabs = (
        key_piece.reshape(steps_count, step_rows, HD),
        value_piece.reshape(steps_count, step_rows, HD),
        key_pos.reshape(steps_count, step_rows),
        key_doc.reshape(steps_count, step_rows),
    )
    result, _ = lax.scan(one_step, start_state, slabs)
    final_max, final_total, final_acc = result
    attention = (final_acc / final_total.T[:, :, None]).reshape(rows, HQ * HD).astype(jnp.bfloat16)
    as_float = student_in.astype(jnp.float32)
    normed = (
        as_float * lax.rsqrt(jnp.mean(as_float * as_float, axis=1, keepdims=True) + EPSILON)
    ).astype(jnp.bfloat16)
    group_rows = lax.all_gather(weight, "seq", axis=0, tiled=True)
    columns = normed
    predicted = jnp.dot(
        columns,
        lax.all_gather(group_rows, "dp", axis=0, tiled=True),
        preferred_element_type=jnp.float32,
    )
    dp_count = lax.axis_size("dp")
    seq_count = lax.axis_size("seq")
    token_total = rows * dp_count * seq_count
    scaled = ((predicted - attention.astype(jnp.float32)) * token_total ** (-0.5)).astype(
        jnp.bfloat16
    )
    columns = normed
    outer_rows = lax.psum_scatter(
        lax.dot_general(
            columns, scaled, (((0,), (0,)), ((), ())), preferred_element_type=jnp.float32
        ).astype(jnp.bfloat16),
        "dp",
        scatter_dimension=0,
        tiled=True,
    )
    weight_grad = lax.psum_scatter(outer_rows, "seq", scatter_dimension=0, tiled=True).astype(
        jnp.float32
    )
    return (attention, weight_grad)


MESH = pl.DeviceIdType.MESH
F32 = jnp.float32
BF16 = jnp.bfloat16


def fused_kernel(
    token_total,
    x_ref, w_ref, q_ref, k_ref, v_ref, len_ref, asg_ref,
    att_ref, out_ref,
    x_peer, w_all, kv_all, xn, xt, pred, att_half, att_peer,
    own_f, gx_f, gy_f, s_d, s_x, s_y, s_z, r_dx, r_dy, r_x, r_y, r_z,
    send, sem_w, sem_kv, sem_x, sem_att, sem_dx, sem_dy, sem_rx, sem_ry, sem_rz,
):
    rows = q_ref.shape[0]
    piece = w_ref.shape[0]
    half = w_ref.shape[1] // 2
    depth = xn.shape[2]
    dp, z = lax.axis_index("dp"), lax.axis_index("seq")
    c = dp % 2
    pc = 1 - c
    x = (dp // 2) % 2
    y = dp // 4
    q = dp // 2
    qx, qy, qd = y * 2 + 1 - x, (1 - y) * 2 + x, 3 - q
    mate = (dp + 1 - 2 * c, z)
    xn_dev = (dp + 2 - 4 * x, z)
    yn_dev = (dp + 4 - 8 * y, z)
    zs = (z, z + 1 - 2 * (z % 2), z + 2 - 4 * (z // 2), 3 - z)
    z_dev = [(dp, zs[r]) for r in range(4)]
    z_mate = [(dp + 1 - 2 * c, zs[r]) for r in range(4)]

    peers = [mate, xn_dev, yn_dev] + z_dev[1:] + z_mate[1:]
    barrier = pltpu.get_barrier_semaphore()
    for dev in peers:
        pl.semaphore_signal(barrier, inc=1, device_id=dev, device_id_type=MESH)
    pl.semaphore_wait(barrier, len(peers))

    sent = []

    def push(src, dst, rsem, dev):
        copy = pltpu.make_async_remote_copy(
            src_ref=src, dst_ref=dst, send_sem=send.at[len(sent)], recv_sem=rsem,
            device_id=dev, device_id_type=MESH,
        )
        copy.start()
        sent.append(copy)

    def arrive(dst, rsem):
        pltpu.make_async_remote_copy(
            src_ref=dst, dst_ref=dst, send_sem=send.at[0], recv_sem=rsem,
            device_id=mate, device_id_type=MESH,
        ).wait_recv()

    def cols(core):
        return pl.ds(pl.multiple_of(core * half, 128), half)

    def w_push(at, dev):
        push(w_all.at[at], w_all.at[at], sem_w.at[at], dev)

    def w_arrive(at):
        arrive(w_all.at[at], sem_w.at[at])

    mine, other = (q, c, z), (q, pc, z)
    own_half = w_ref.at[:, cols(c)]
    push(w_ref.at[:, cols(pc)], w_all.at[mine], sem_w.at[mine], mate)
    for dev in (z_dev[1], xn_dev, yn_dev):
        push(own_half, w_all.at[mine], sem_w.at[mine], dev)
    push(x_ref, x_peer, sem_x.at[0], mate)
    w_all[mine] = w_ref[:, cols(c)]
    w_arrive(other)
    for dev in (z_dev[1], xn_dev, yn_dev):
        w_push(other, dev)
    for r in (2, 3):
        push(own_half, w_all.at[mine], sem_w.at[mine], z_dev[r])
        w_push(other, z_dev[r])
        if r == 2:
            kv_push_order = (1,)
        else:
            kv_push_order = (2, 3)
        for s in kv_push_order:
            push(k_ref, kv_all.at[0, z], sem_kv.at[0, z], z_dev[s])
            push(v_ref, kv_all.at[1, z], sem_kv.at[1, z], z_dev[s])
    kv_all[0, z] = k_ref[...]
    kv_all[1, z] = v_ref[...]

    step = 16

    def norm_rows(source, base):
        @pl.loop(0, rows // step)
        def _(i):
            at = pl.multiple_of(i * step, step)
            block = source[pl.ds(at, step), :].astype(F32)
            normed = (
                block * lax.rsqrt(jnp.mean(block * block, axis=1, keepdims=True) + EPSILON)
            ).astype(BF16)
            for part in range(4):
                xn[part, pl.ds(pl.multiple_of(base + at, step), step), :] = normed[
                    :, part * depth : (part + 1) * depth
                ]

    def relay(r):
        w_arrive((qx, 0, zs[r]))
        w_push((qx, 0, zs[r]), yn_dev)
        w_arrive((qy, 1, zs[r]))
        w_push((qy, 1, zs[r]), xn_dev)

    def forward(r):
        for part in range(2):
            at = (q, part, zs[r])
            w_arrive(at)
            w_push(at, xn_dev)
            w_push(at, yn_dev)

    def w_block(at):
        return w_all[at].reshape(depth, half)

    norm_rows(x_ref, 0)
    relay(0)
    forward(1)
    arrive(x_peer, sem_x.at[0])
    norm_rows(x_peer, rows)
    forward(2)
    relay(1)

    @pl.loop(0, 4)
    def _(part):
        for j in range(depth // 128):
            xt[part, j * 128 : (j + 1) * 128, :] = xn[part, :, j * 128 : (j + 1) * 128].T

    forward(3)
    relay(2)
    pred[...] = jnp.dot(xn[q], w_block(q), preferred_element_type=F32)

    for r in range(1, 4):
        for part in range(2):
            arrive(kv_all.at[part, zs[r]], sem_kv.at[part, zs[r]])
    ends = []
    total = 0
    for i in range(len_ref.shape[1]):
        total = total + len_ref[0, i]
        ends.append(total)

    def document(position):
        found = jnp.zeros(position.shape, jnp.int32)
        for end in ends:
            found = found + (position >= end).astype(jnp.int32)
        return found

    lanes = lax.broadcasted_iota(jnp.int32, (1, BLK), 1)
    k_pos = jnp.concatenate([asg_ref[0, j] * BLK + lanes for j in range(4)], axis=1)
    q_pos = asg_ref[0, z] * BLK + lax.broadcasted_iota(jnp.int32, (rows, 1), 0)
    allowed = (document(q_pos) == document(k_pos)) & (q_pos >= k_pos)
    k_all = kv_all[0].reshape(4 * rows, HD)
    v_all = kv_all[1].reshape(4 * rows, HD)
    for h in range(HQ):
        scores = lax.dot_general(
            q_ref[:, h * HD : (h + 1) * HD], k_all, (((1,), (1,)), ((), ())),
            preferred_element_type=F32,
        ) * HD ** (-0.5)
        masked = jnp.where(allowed, scores, NEGATIVE)
        top = jnp.max(masked, axis=1, keepdims=True)
        terms = jnp.where(allowed, jnp.exp(masked - top), 0.0)
        totals = jnp.sum(terms, axis=1, keepdims=True)
        mixture = jnp.dot(terms.astype(BF16), v_all, preferred_element_type=F32)
        done = (mixture / totals).astype(BF16)
        att_ref[:, h * HD : (h + 1) * HD] = done
        place = (h % 2) * HD
        att_half[h // 2, :, place : place + HD] = done
    push(att_half.at[pc], att_peer, sem_att.at[0], mate)
    relay(3)

    for r in range(4):
        w_arrive((qx, 1, zs[r]))
    pred[...] += jnp.dot(xn[qx], w_block(qx), preferred_element_type=F32)
    for r in range(4):
        w_arrive((qy, 0, zs[r]))
    pred[...] += jnp.dot(xn[qy], w_block(qy), preferred_element_type=F32)
    arrive(att_peer, sem_att.at[0])
    for r in range(4):
        for part in range(2):
            w_arrive((qd, part, zs[r]))
    predicted = pred[...] + jnp.dot(xn[qd], w_block(qd), preferred_element_type=F32)
    attended = jnp.concatenate([att_half[c], att_peer[...]], axis=0).astype(F32)
    scaled = ((predicted - attended) * token_total ** (-0.5)).astype(BF16)

    def grad(at):
        return jnp.dot(xt[at], scaled, preferred_element_type=F32).reshape(2, 4, piece, half)

    def send_diagonal(g):
        push(s_d.at[0, g], r_dy.at[g], sem_dy.at[g], yn_dev)
        push(s_d.at[1, g], r_dx.at[g], sem_dx.at[g], xn_dev)

    def send_direct(g):
        push(s_x.at[1, g], r_x.at[1, g], sem_rx.at[1, g], xn_dev)
        push(s_y.at[0, g], r_y.at[0, g], sem_ry.at[0, g], yn_dev)

    def send_joined(g):
        arrive(r_dy.at[g], sem_dy.at[g])
        s_x[0, g] = (gx_f[g] + r_dy[g].astype(F32)).astype(BF16)
        push(s_x.at[0, g], r_x.at[0, g], sem_rx.at[0, g], xn_dev)
        arrive(r_dx.at[g], sem_dx.at[g])
        s_y[1, g] = (gy_f[g] + r_dx[g].astype(F32)).astype(BF16)
        push(s_y.at[1, g], r_y.at[1, g], sem_ry.at[1, g], yn_dev)

    def column_sum(part, g):
        arrive(r_x.at[part, g], sem_rx.at[part, g])
        arrive(r_y.at[part, g], sem_ry.at[part, g])
        return own_f[part, g] + r_x[part, g].astype(F32) + r_y[part, g].astype(F32)

    def send_column(r):
        g = zs[r]
        for part in range(2):
            s_z[part, g] = column_sum(part, g).astype(BF16)
        push(s_z.at[c, g], r_z.at[z, c], sem_rz.at[z, c], z_dev[r])
        push(s_z.at[pc, g], r_z.at[z, c], sem_rz.at[z, c], z_mate[r])

    order = (3, 2, 1, 0)
    g = [zs[r] for r in order]
    s_d[...] = grad(qd).astype(BF16)
    send_diagonal(g[0])
    send_diagonal(g[1])
    block = grad(qx)
    gx_f[...] = block[0]
    s_x[1] = block[1].astype(BF16)
    block = grad(qy)
    gy_f[...] = block[1]
    s_y[0] = block[0].astype(BF16)
    send_direct(g[0])
    own_f[...] = grad(q)
    send_joined(g[0])
    send_diagonal(g[2])
    send_direct(g[1])
    send_joined(g[1])
    send_diagonal(g[3])
    send_direct(g[2])
    send_column(order[0])
    send_joined(g[2])
    send_direct(g[3])
    send_column(order[1])
    send_joined(g[3])
    send_column(order[2])

    for part in range(2):
        own_f[part, z] = column_sum(part, z)
    s_z[pc, z] = own_f[pc, z].astype(BF16)
    push(s_z.at[pc, z], r_z.at[z, c], sem_rz.at[z, c], mate)
    total = own_f[c, z]
    for r in range(1, 4):
        arrive(r_z.at[zs[r], c], sem_rz.at[zs[r], c])
        total = total + r_z[zs[r], c].astype(F32)
    out_ref[:, cols(c)] = total
    total = jnp.zeros((piece, half), F32)
    for r in (3, 2, 1, 0):
        arrive(r_z.at[zs[r], pc], sem_rz.at[zs[r], pc])
        total = total + r_z[zs[r], pc].astype(F32)
    out_ref[:, cols(pc)] = total
    for copy in sent:
        copy.wait_send()


def local_fused(student_in, weight, queries, keys, values, lengths, assignment):
    rows, width = student_in.shape
    piece, features = weight.shape
    half = features // 2
    depth = width // 4
    token_total = rows * lax.axis_size("dp") * lax.axis_size("seq")
    vmem = pl.BlockSpec(memory_space=pltpu.VMEM)
    smem = pl.BlockSpec(memory_space=pltpu.SMEM)
    dma = pltpu.SemaphoreType.DMA
    quarter = (2, 4, piece, half)
    return pl.pallas_call(
        functools.partial(fused_kernel, token_total),
        out_shape=(
            jax.ShapeDtypeStruct((rows, features), BF16),
            jax.ShapeDtypeStruct((piece, features), F32),
        ),
        in_specs=[vmem] * 5 + [smem] * 2,
        out_specs=(vmem, vmem),
        scratch_shapes=[
            pltpu.VMEM((rows, width), BF16),
            pltpu.VMEM((4,) + quarter, BF16),
            pltpu.VMEM((2, 4, rows, HD), BF16),
            pltpu.VMEM((4, 2 * rows, depth), BF16),
            pltpu.VMEM((4, depth, 2 * rows), BF16),
            pltpu.VMEM((2 * rows, half), F32),
            pltpu.VMEM((2, rows, half), BF16),
            pltpu.VMEM((rows, half), BF16),
            pltpu.VMEM(quarter, F32),
            pltpu.VMEM(quarter[1:], F32),
            pltpu.VMEM(quarter[1:], F32),
            pltpu.VMEM(quarter, BF16),
            pltpu.VMEM(quarter, BF16),
            pltpu.VMEM(quarter, BF16),
            pltpu.VMEM(quarter, BF16),
            pltpu.VMEM(quarter[1:], BF16),
            pltpu.VMEM(quarter[1:], BF16),
            pltpu.VMEM(quarter, BF16),
            pltpu.VMEM(quarter, BF16),
            pltpu.VMEM((4, 2, piece, half), BF16),
            dma((80,)),
            dma((4, 2, 4)),
            dma((2, 4)),
            dma((1,)),
            dma((1,)),
            dma((4,)),
            dma((4,)),
            dma((2, 4)),
            dma((2, 4)),
            dma((4, 2)),
        ],
        compiler_params=pltpu.CompilerParams(collective_id=0, has_side_effects=True),
        name="distill",
    )(student_in, weight, queries, keys, values, lengths, assignment)


def fits(student_in, weight, queries, keys, values, lengths, assignment):
    rows, width = student_in.shape
    piece, features = weight.shape
    return (
        lax.axis_size("dp") == 8
        and lax.axis_size("seq") == 4
        and rows == BLK
        and assignment.shape[1] == 4
        and piece % 16 == 0
        and width == 32 * piece
        and width % 512 == 0
        and features == HQ * HD
        and keys.shape[1] == HD
    )


def dispatch(*arrays):
    return local_fused(*arrays) if fits(*arrays) else local(*arrays)


def solution(mesh):
    placed = (
        P(("dp", "seq"), None),
        P(("dp", "seq"), None),
        P(("dp", "seq"), None),
        P(("dp", "seq"), None),
        P(("dp", "seq"), None),
        P("dp", None),
        P("dp", None),
    )
    return jax.shard_map(
        dispatch,
        mesh=mesh,
        in_specs=placed,
        out_specs=(P(("dp", "seq"), None), P(("dp", "seq"), None)),
        check_vma=False,
    )
```

```python
import functools
import math

import jax
import jax.numpy as jnp
from jax import lax
from jax.experimental import pallas as pl
from jax.experimental.pallas import tpu as pltpu
from jax.sharding import PartitionSpec as P

HD = 128
HQ = 4
BLK = 128


EPSILON = 1e-06
NEGATIVE = -1e30


def locate(assign_row, doc_ends, first_slot, count):
    slot_ids = first_slot + jnp.arange(count, dtype=jnp.int32)
    block_ids = slot_ids // BLK
    block_table = jnp.arange(assign_row.shape[0], dtype=jnp.int32)
    placed = jnp.sum(
        jnp.where(block_ids[:, None] == block_table[None, :], assign_row[None, :], 0), axis=1
    )
    position = placed * BLK + slot_ids % BLK
    document = jnp.sum((position[:, None] >= doc_ends[None, :]).astype(jnp.int32), axis=1)
    return (position, document)


def absorb_block(state, key_block, value_block, query_heads, allowed):
    run_max, run_total, run_acc = state
    scores = jnp.einsum(
        "qhd,kd->hqk", query_heads, key_block, preferred_element_type=jnp.float32
    ) * HD ** (-0.5)
    masked = jnp.where(allowed[None], scores, NEGATIVE)
    new_max = jnp.maximum(run_max, jnp.max(masked, axis=-1))
    fading = jnp.exp(run_max - new_max)
    exp_terms = jnp.where(allowed[None], jnp.exp(masked - new_max[:, :, None]), 0.0)
    new_total = run_total * fading + jnp.sum(exp_terms, axis=-1)
    mixture = jnp.einsum(
        "hqk,kd->qhd",
        exp_terms.astype(jnp.bfloat16),
        value_block,
        preferred_element_type=jnp.float32,
    )
    new_acc = run_acc * fading.T[:, :, None] + mixture
    return (new_max, new_total, new_acc)


def local(student_in, weight, queries, keys, values, lengths, assignment):
    rows = queries.shape[0]
    assign_row = assignment[0]
    doc_ends = jnp.cumsum(lengths[0])
    query_pos, query_doc = locate(assign_row, doc_ends, lax.axis_index("seq") * rows, rows)
    query_heads = queries.reshape(rows, HQ, HD)
    start_state = (
        jnp.full((HQ, rows), NEGATIVE, jnp.float32),
        jnp.zeros((HQ, rows), jnp.float32),
        jnp.zeros((rows, HQ, HD), jnp.float32),
    )
    key_piece = lax.all_gather(keys, "seq", axis=0, tiled=True)
    value_piece = lax.all_gather(values, "seq", axis=0, tiled=True)
    count = key_piece.shape[0]
    step_rows = math.gcd(count, 512)
    steps_count = count // step_rows
    key_pos, key_doc = locate(assign_row, doc_ends, jnp.int32(0), count)

    def one_step(running, slabs):
        key_block, value_block, key_position, key_document = slabs
        allowed = (query_doc[:, None] == key_document[None, :]) & (
            query_pos[:, None] >= key_position[None, :]
        )
        updated = absorb_block(running, key_block, value_block, query_heads, allowed)
        return (updated, None)

    slabs = (
        key_piece.reshape(steps_count, step_rows, HD),
        value_piece.reshape(steps_count, step_rows, HD),
        key_pos.reshape(steps_count, step_rows),
        key_doc.reshape(steps_count, step_rows),
    )
    result, _ = lax.scan(one_step, start_state, slabs)
    final_max, final_total, final_acc = result
    attention = (final_acc / final_total.T[:, :, None]).reshape(rows, HQ * HD).astype(jnp.bfloat16)
    as_float = student_in.astype(jnp.float32)
    normed = (
        as_float * lax.rsqrt(jnp.mean(as_float * as_float, axis=1, keepdims=True) + EPSILON)
    ).astype(jnp.bfloat16)
    group_rows = lax.all_gather(weight, "seq", axis=0, tiled=True)
    columns = normed
    predicted = jnp.dot(
        columns,
        lax.all_gather(group_rows, "dp", axis=0, tiled=True),
        preferred_element_type=jnp.float32,
    )
    dp_count = lax.axis_size("dp")
    seq_count = lax.axis_size("seq")
    token_total = rows * dp_count * seq_count
    scaled = ((predicted - attention.astype(jnp.float32)) * token_total ** (-0.5)).astype(
        jnp.bfloat16
    )
    columns = normed
    outer_rows = lax.psum_scatter(
        lax.dot_general(
            columns, scaled, (((0,), (0,)), ((), ())), preferred_element_type=jnp.float32
        ).astype(jnp.bfloat16),
        "dp",
        scatter_dimension=0,
        tiled=True,
    )
    weight_grad = lax.psum_scatter(outer_rows, "seq", scatter_dimension=0, tiled=True).astype(
        jnp.float32
    )
    return (attention, weight_grad)


MESH = pl.DeviceIdType.MESH
F32 = jnp.float32
BF16 = jnp.bfloat16


def fused_kernel(
    token_total,
    x_ref, w_ref, q_ref, k_ref, v_ref, len_ref, asg_ref,
    att_ref, out_ref,
    xs, xt, w_all, kv_all, inv, pred, p_out, p_in, s_all, att_half, att_peer,
    grad_f, s_y, r_y, s_z, r_z,
    send, sem_w, sem_kv, sem_x, sem_inv, sem_att, sem_p, sem_s, sem_ry, sem_rz,
):
    rows = q_ref.shape[0]
    piece = w_ref.shape[0]
    half = w_ref.shape[1] // 2
    depth = xs.shape[3]
    dp, z = lax.axis_index("dp"), lax.axis_index("seq")
    c = dp % 2
    pc = 1 - c
    x = (dp // 2) % 2
    y = dp // 4
    yo = 1 - y
    mate = (dp + 1 - 2 * c, z)
    xn_dev = (dp + 2 - 4 * x, z)
    yn_dev = (dp + 4 - 8 * y, z)
    zs = (z, z + 1 - 2 * (z % 2), z + 2 - 4 * (z // 2), 3 - z)
    z_dev = [(dp, zs[r]) for r in range(4)]
    z_mate = [(dp + 1 - 2 * c, zs[r]) for r in range(4)]

    peers = [mate, xn_dev, yn_dev] + z_dev[1:] + z_mate[1:]
    barrier = pltpu.get_barrier_semaphore()
    for dev in peers:
        pl.semaphore_signal(barrier, inc=1, device_id=dev, device_id_type=MESH)
    pl.semaphore_wait(barrier, len(peers))

    sent = []

    def push(src, dst, rsem, dev):
        copy = pltpu.make_async_remote_copy(
            src_ref=src, dst_ref=dst, send_sem=send.at[len(sent)], recv_sem=rsem,
            device_id=dev, device_id_type=MESH,
        )
        copy.start()
        sent.append(copy)

    def arrive(dst, rsem):
        pltpu.make_async_remote_copy(
            src_ref=dst, dst_ref=dst, send_sem=send.at[0], recv_sem=rsem,
            device_id=mate, device_id_type=MESH,
        ).wait_recv()

    def cols(core):
        return pl.ds(pl.multiple_of(core * half, 128), half)

    def width(at_y, at_x):
        return pl.ds(pl.multiple_of((at_y * 2 + at_x) * depth, 128), depth)

    def w_push(at, dev):
        push(w_all.at[at], w_all.at[at], sem_w.at[at], dev)

    def w_arrive(at):
        arrive(w_all.at[at], sem_w.at[at])

    def x_push(at_y, at_x, slot, dev):
        push(x_ref.at[:, width(at_y, at_x)], xs.at[at_y, slot], sem_x.at[at_y, slot], dev)

    mine, other = (y, c, z), (y, pc, z)
    own_half = w_ref.at[:, cols(c)]
    push(w_ref.at[:, cols(pc)], w_all.at[mine], sem_w.at[mine], mate)
    push(own_half, w_all.at[mine], sem_w.at[mine], z_dev[1])
    push(own_half, w_all.at[mine], sem_w.at[mine], yn_dev)
    x_push(y, 1 - x, 2, xn_dev)
    x_push(yo, 1 - x, 2, xn_dev)
    x_push(y, x, 1, mate)
    x_push(yo, x, 1, mate)
    w_all[mine] = w_ref[:, cols(c)]
    w_arrive(other)
    w_push(other, z_dev[1])
    w_push(other, yn_dev)
    for r in (2, 3):
        push(own_half, w_all.at[mine], sem_w.at[mine], z_dev[r])
        w_push(other, z_dev[r])
    for r in (1, 2, 3):
        push(k_ref, kv_all.at[0, z], sem_kv.at[0, z], z_dev[r])
        push(v_ref, kv_all.at[1, z], sem_kv.at[1, z], z_dev[r])
    kv_all[0, z] = k_ref[...]
    kv_all[1, z] = v_ref[...]
    xs[y, 0] = x_ref[:, width(y, x)]
    xs[yo, 0] = x_ref[:, width(yo, x)]

    step = 16

    @pl.loop(0, rows // step)
    def _(i):
        at = pl.ds(pl.multiple_of(i * step, step), step)
        block = x_ref[at, :].astype(F32)
        factor = lax.rsqrt(jnp.mean(block * block, axis=1, keepdims=True) + EPSILON)
        inv[0, at, :] = jnp.broadcast_to(factor, (step, 128))

    push(inv.at[0], inv.at[1], sem_inv.at[0], mate)

    def forward(r):
        for part in range(2):
            at = (y, part, zs[r])
            w_arrive(at)
            w_push(at, yn_dev)

    def x_arrive(at_y, slot):
        arrive(xs.at[at_y, slot], sem_x.at[at_y, slot])

    def x_relay(at_y):
        x_arrive(at_y, 2)
        push(xs.at[at_y, 2], xs.at[at_y, 3], sem_x.at[at_y, 3], mate)

    def turn(at_y, slot):
        for j in range(depth // 128):
            at = slice(j * 128, (j + 1) * 128)
            xt[at_y, at, slot * rows : (slot + 1) * rows] = xs[at_y, slot, :, at].T

    def w_block(at_y):
        return w_all[at_y].reshape(depth, half)

    def product(at_y, first):
        return jnp.dot(
            xs[at_y, first : first + 2].reshape(2 * rows, depth), w_block(at_y),
            preferred_element_type=F32,
        )

    forward(1)
    x_arrive(y, 1)
    x_arrive(yo, 1)
    for slot in range(2):

        @pl.loop(0, 2)
        def _(at_y):
            turn(at_y, slot)

    forward(2)
    x_relay(y)
    forward(3)
    pred[0] = product(y, 0)
    x_relay(yo)
    x_arrive(y, 3)
    pred[1] = product(y, 2)
    turn(y, 2)
    turn(y, 3)
    x_arrive(yo, 3)
    for r in range(4):
        for part in range(2):
            w_arrive((yo, part, zs[r]))
    p_out[...] = (pred[1] + product(yo, 2)).astype(BF16).reshape(2, rows, half)
    for slot in range(2):
        push(p_out.at[slot], p_in.at[slot], sem_p.at[slot], xn_dev)
    pred[0] += product(yo, 0)

    for r in range(1, 4):
        for part in range(2):
            arrive(kv_all.at[part, zs[r]], sem_kv.at[part, zs[r]])
    ends = []
    total = 0
    for i in range(len_ref.shape[1]):
        total = total + len_ref[0, i]
        ends.append(total)

    def document(position):
        found = jnp.zeros(position.shape, jnp.int32)
        for end in ends:
            found = found + (position >= end).astype(jnp.int32)
        return found

    lanes = lax.broadcasted_iota(jnp.int32, (1, BLK), 1)
    k_pos = jnp.concatenate([asg_ref[0, j] * BLK + lanes for j in range(4)], axis=1)
    q_pos = asg_ref[0, z] * BLK + lax.broadcasted_iota(jnp.int32, (rows, 1), 0)
    allowed = (document(q_pos) == document(k_pos)) & (q_pos >= k_pos)
    k_all = kv_all[0].reshape(4 * rows, HD)
    v_all = kv_all[1].reshape(4 * rows, HD)
    for h in range(HQ):
        scores = lax.dot_general(
            q_ref[:, h * HD : (h + 1) * HD], k_all, (((1,), (1,)), ((), ())),
            preferred_element_type=F32,
        ) * HD ** (-0.5)
        masked = jnp.where(allowed, scores, NEGATIVE)
        top = jnp.max(masked, axis=1, keepdims=True)
        terms = jnp.where(allowed, jnp.exp(masked - top), 0.0)
        totals = jnp.sum(terms, axis=1, keepdims=True)
        mixture = jnp.dot(terms.astype(BF16), v_all, preferred_element_type=F32)
        done = (mixture / totals).astype(BF16)
        att_ref[:, h * HD : (h + 1) * HD] = done
        place = (h % 2) * HD
        att_half[h // 2, :, place : place + HD] = done
    push(att_half.at[pc], att_peer, sem_att.at[0], mate)

    def scale_rows(slot, attended):
        arrive(p_in.at[slot], sem_p.at[slot])
        factor = jnp.concatenate([inv[slot]] * (half // 128), axis=1)
        raw = pred[0, slot * rows : (slot + 1) * rows, :] + p_in[slot].astype(F32)
        gap = raw * factor - attended.astype(F32)
        s_all[slot] = (gap * token_total ** (-0.5) * factor).astype(BF16)
        push(s_all.at[slot], s_all.at[slot + 2], sem_s.at[slot], xn_dev)

    scale_rows(0, att_half[c])
    arrive(att_peer, sem_att.at[0])
    arrive(inv.at[1], sem_inv.at[0])
    scale_rows(1, att_peer[...])
    turn(yo, 2)
    turn(yo, 3)

    def grad(at_y, first):
        return jnp.dot(
            xt[at_y, :, first * rows : (first + 2) * rows],
            s_all[first : first + 2].reshape(2 * rows, half),
            preferred_element_type=F32,
        ).reshape(2, 4, piece, half)

    grad_f[yo] = grad(yo, 0)
    grad_f[y] = grad(y, 0)
    for slot in range(2):
        arrive(s_all.at[slot + 2], sem_s.at[slot])
    s_y[...] = (grad_f[yo] + grad(yo, 2)).astype(BF16)
    order = (3, 2, 1, 0)
    for r in order:
        for part in range(2):
            at = (part, zs[r])
            push(s_y.at[at], r_y.at[at], sem_ry.at[at], yn_dev)
    grad_f[y] += grad(y, 2)

    def column_sum(part, g):
        arrive(r_y.at[part, g], sem_ry.at[part, g])
        return grad_f[y, part, g] + r_y[part, g].astype(F32)

    for r in order[:3]:
        g = zs[r]
        for part in range(2):
            s_z[part, g] = column_sum(part, g).astype(BF16)
        push(s_z.at[c, g], r_z.at[z, c], sem_rz.at[z, c], z_dev[r])
        push(s_z.at[pc, g], r_z.at[z, c], sem_rz.at[z, c], z_mate[r])
    for part in range(2):
        grad_f[y, part, z] = column_sum(part, z)
    s_z[pc, z] = grad_f[y, pc, z].astype(BF16)
    push(s_z.at[pc, z], r_z.at[z, c], sem_rz.at[z, c], mate)
    total = grad_f[y, c, z]
    for r in range(1, 4):
        arrive(r_z.at[zs[r], c], sem_rz.at[zs[r], c])
        total = total + r_z[zs[r], c].astype(F32)
    out_ref[:, cols(c)] = total
    total = jnp.zeros((piece, half), F32)
    for r in (3, 2, 1, 0):
        arrive(r_z.at[zs[r], pc], sem_rz.at[zs[r], pc])
        total = total + r_z[zs[r], pc].astype(F32)
    out_ref[:, cols(pc)] = total
    for copy in sent:
        copy.wait_send()


def local_fused(student_in, weight, queries, keys, values, lengths, assignment):
    rows, width = student_in.shape
    piece, features = weight.shape
    half = features // 2
    depth = width // 4
    token_total = rows * lax.axis_size("dp") * lax.axis_size("seq")
    vmem = pl.BlockSpec(memory_space=pltpu.VMEM)
    smem = pl.BlockSpec(memory_space=pltpu.SMEM)
    dma = pltpu.SemaphoreType.DMA
    quarter = (2, 4, piece, half)
    return pl.pallas_call(
        functools.partial(fused_kernel, token_total),
        out_shape=(
            jax.ShapeDtypeStruct((rows, features), BF16),
            jax.ShapeDtypeStruct((piece, features), F32),
        ),
        in_specs=[vmem] * 5 + [smem] * 2,
        out_specs=(vmem, vmem),
        scratch_shapes=[
            pltpu.VMEM((2, 4, rows, depth), BF16),
            pltpu.VMEM((2, depth, 4 * rows), BF16),
            pltpu.VMEM((2,) + quarter, BF16),
            pltpu.VMEM((2, 4, rows, HD), BF16),
            pltpu.VMEM((2, rows, 128), F32),
            pltpu.VMEM((2, 2 * rows, half), F32),
            pltpu.VMEM((2, rows, half), BF16),
            pltpu.VMEM((2, rows, half), BF16),
            pltpu.VMEM((4, rows, half), BF16),
            pltpu.VMEM((2, rows, half), BF16),
            pltpu.VMEM((rows, half), BF16),
            pltpu.VMEM((2,) + quarter, F32),
            pltpu.VMEM(quarter, BF16),
            pltpu.VMEM(quarter, BF16),
            pltpu.VMEM(quarter, BF16),
            pltpu.VMEM((4, 2, piece, half), BF16),
            dma((64,)),
            dma((2, 2, 4)),
            dma((2, 4)),
            dma((2, 4)),
            dma((1,)),
            dma((1,)),
            dma((2,)),
            dma((2,)),
            dma((2, 4)),
            dma((4, 2)),
        ],
        compiler_params=pltpu.CompilerParams(collective_id=0, has_side_effects=True),
        name="distill",
    )(student_in, weight, queries, keys, values, lengths, assignment)


def fits(student_in, weight, queries, keys, values, lengths, assignment):
    rows, width = student_in.shape
    piece, features = weight.shape
    return (
        lax.axis_size("dp") == 8
        and lax.axis_size("seq") == 4
        and rows == BLK
        and assignment.shape[1] == 4
        and piece % 16 == 0
        and width == 32 * piece
        and width % 512 == 0
        and features == HQ * HD
        and keys.shape[1] == HD
    )


def dispatch(*arrays):
    return local_fused(*arrays) if fits(*arrays) else local(*arrays)


def solution(mesh):
    placed = (
        P(("dp", "seq"), None),
        P(("dp", "seq"), None),
        P(("dp", "seq"), None),
        P(("dp", "seq"), None),
        P(("dp", "seq"), None),
        P("dp", None),
        P("dp", None),
    )
    return jax.shard_map(
        dispatch,
        mesh=mesh,
        in_specs=placed,
        out_specs=(P(("dp", "seq"), None), P(("dp", "seq"), None)),
        check_vma=False,
    )
```

```python
import functools
import math

import jax
import jax.numpy as jnp
from jax import lax
from jax.experimental import pallas as pl
from jax.experimental.pallas import tpu as pltpu
from jax.sharding import PartitionSpec as P

HD = 128
HQ = 4
BLK = 128


EPSILON = 1e-06
NEGATIVE = -1e30


def locate(assign_row, doc_ends, first_slot, count):
    slot_ids = first_slot + jnp.arange(count, dtype=jnp.int32)
    block_ids = slot_ids // BLK
    block_table = jnp.arange(assign_row.shape[0], dtype=jnp.int32)
    placed = jnp.sum(
        jnp.where(block_ids[:, None] == block_table[None, :], assign_row[None, :], 0), axis=1
    )
    position = placed * BLK + slot_ids % BLK
    document = jnp.sum((position[:, None] >= doc_ends[None, :]).astype(jnp.int32), axis=1)
    return (position, document)


def absorb_block(state, key_block, value_block, query_heads, allowed):
    run_max, run_total, run_acc = state
    scores = jnp.einsum(
        "qhd,kd->hqk", query_heads, key_block, preferred_element_type=jnp.float32
    ) * HD ** (-0.5)
    masked = jnp.where(allowed[None], scores, NEGATIVE)
    new_max = jnp.maximum(run_max, jnp.max(masked, axis=-1))
    fading = jnp.exp(run_max - new_max)
    exp_terms = jnp.where(allowed[None], jnp.exp(masked - new_max[:, :, None]), 0.0)
    new_total = run_total * fading + jnp.sum(exp_terms, axis=-1)
    mixture = jnp.einsum(
        "hqk,kd->qhd",
        exp_terms.astype(jnp.bfloat16),
        value_block,
        preferred_element_type=jnp.float32,
    )
    new_acc = run_acc * fading.T[:, :, None] + mixture
    return (new_max, new_total, new_acc)


def local(student_in, weight, queries, keys, values, lengths, assignment):
    rows = queries.shape[0]
    assign_row = assignment[0]
    doc_ends = jnp.cumsum(lengths[0])
    query_pos, query_doc = locate(assign_row, doc_ends, lax.axis_index("seq") * rows, rows)
    query_heads = queries.reshape(rows, HQ, HD)
    start_state = (
        jnp.full((HQ, rows), NEGATIVE, jnp.float32),
        jnp.zeros((HQ, rows), jnp.float32),
        jnp.zeros((rows, HQ, HD), jnp.float32),
    )
    key_piece = lax.all_gather(keys, "seq", axis=0, tiled=True)
    value_piece = lax.all_gather(values, "seq", axis=0, tiled=True)
    count = key_piece.shape[0]
    step_rows = math.gcd(count, 512)
    steps_count = count // step_rows
    key_pos, key_doc = locate(assign_row, doc_ends, jnp.int32(0), count)

    def one_step(running, slabs):
        key_block, value_block, key_position, key_document = slabs
        allowed = (query_doc[:, None] == key_document[None, :]) & (
            query_pos[:, None] >= key_position[None, :]
        )
        updated = absorb_block(running, key_block, value_block, query_heads, allowed)
        return (updated, None)

    slabs = (
        key_piece.reshape(steps_count, step_rows, HD),
        value_piece.reshape(steps_count, step_rows, HD),
        key_pos.reshape(steps_count, step_rows),
        key_doc.reshape(steps_count, step_rows),
    )
    result, _ = lax.scan(one_step, start_state, slabs)
    final_max, final_total, final_acc = result
    attention = (final_acc / final_total.T[:, :, None]).reshape(rows, HQ * HD).astype(jnp.bfloat16)
    as_float = student_in.astype(jnp.float32)
    normed = (
        as_float * lax.rsqrt(jnp.mean(as_float * as_float, axis=1, keepdims=True) + EPSILON)
    ).astype(jnp.bfloat16)
    group_rows = lax.all_gather(weight, "seq", axis=0, tiled=True)
    columns = normed
    predicted = jnp.dot(
        columns,
        lax.all_gather(group_rows, "dp", axis=0, tiled=True),
        preferred_element_type=jnp.float32,
    )
    dp_count = lax.axis_size("dp")
    seq_count = lax.axis_size("seq")
    token_total = rows * dp_count * seq_count
    scaled = ((predicted - attention.astype(jnp.float32)) * token_total ** (-0.5)).astype(
        jnp.bfloat16
    )
    columns = normed
    outer_rows = lax.psum_scatter(
        lax.dot_general(
            columns, scaled, (((0,), (0,)), ((), ())), preferred_element_type=jnp.float32
        ).astype(jnp.bfloat16),
        "dp",
        scatter_dimension=0,
        tiled=True,
    )
    weight_grad = lax.psum_scatter(outer_rows, "seq", scatter_dimension=0, tiled=True).astype(
        jnp.float32
    )
    return (attention, weight_grad)


MESH = pl.DeviceIdType.MESH
F32 = jnp.float32
BF16 = jnp.bfloat16


def fused_kernel(
    token_total,
    x_ref, w_ref, q_ref, k_ref, v_ref, len_ref, asg_ref,
    att_ref, out_ref,
    xs, xt, w_all, kv_all, inv, pred, p_out, p_in, s_all, att_half, att_peer,
    grad_f, s_y, r_y, s_z, r_z,
    send, send_z, sem_w, sem_kv, sem_x, sem_inv, sem_att, sem_p, sem_s, sem_ry, sem_rz,
):
    rows = q_ref.shape[0]
    piece = w_ref.shape[0]
    half = w_ref.shape[1] // 2
    depth = xs.shape[3]
    dp, z = lax.axis_index("dp"), lax.axis_index("seq")
    c = dp % 2
    pc = 1 - c
    x = (dp // 2) % 2
    y = dp // 4
    yo = 1 - y
    mate = (dp + 1 - 2 * c, z)
    xn_dev = (dp + 2 - 4 * x, z)
    yn_dev = (dp + 4 - 8 * y, z)
    zs = (z, z + 1 - 2 * (z % 2), z + 2 - 4 * (z // 2), 3 - z)
    z_dev = [(dp, zs[r]) for r in range(4)]
    z_mate = [(dp + 1 - 2 * c, zs[r]) for r in range(4)]

    below, above = (dp, (z + 3) % 4), (dp, (z + 1) % 4)
    barrier = pltpu.get_barrier_semaphore()
    for dev in (mate, xn_dev, yn_dev):
        pl.semaphore_signal(barrier, inc=1, device_id=dev, device_id_type=MESH)
    for present, dev in ((z > 0, below), (z < 3, above)):

        @pl.when(present)
        def _():
            pl.semaphore_signal(barrier, inc=1, device_id=dev, device_id_type=MESH)

    pl.semaphore_wait(barrier, 3 + jnp.minimum(z, 1) + jnp.minimum(3 - z, 1))

    sent = []
    sent_when = []

    def push_when(present, src, dst, rsem, dev):
        copy = pltpu.make_async_remote_copy(
            src_ref=src, dst_ref=dst, send_sem=send_z.at[len(sent_when)], recv_sem=rsem,
            device_id=dev, device_id_type=MESH,
        )
        pl.when(present)(copy.start)
        sent_when.append((present, copy))

    def both_ways(src, dst, rsem):
        push_when(z > 0, src, dst, rsem, below)
        push_when(z < 3, src, dst, rsem, above)

    def push(src, dst, rsem, dev):
        copy = pltpu.make_async_remote_copy(
            src_ref=src, dst_ref=dst, send_sem=send.at[len(sent)], recv_sem=rsem,
            device_id=dev, device_id_type=MESH,
        )
        copy.start()
        sent.append(copy)

    def arrive(dst, rsem):
        pltpu.make_async_remote_copy(
            src_ref=dst, dst_ref=dst, send_sem=send.at[0], recv_sem=rsem,
            device_id=mate, device_id_type=MESH,
        ).wait_recv()

    def cols(core):
        return pl.ds(pl.multiple_of(core * half, 128), half)

    def width(at_y, at_x):
        return pl.ds(pl.multiple_of((at_y * 2 + at_x) * depth, 128), depth)

    def w_push(at, dev):
        push(w_all.at[at], w_all.at[at], sem_w.at[at], dev)

    def w_arrive(at):
        arrive(w_all.at[at], sem_w.at[at])

    def x_push(at_y, at_x, slot, dev):
        push(x_ref.at[:, width(at_y, at_x)], xs.at[at_y, slot], sem_x.at[at_y, slot], dev)

    mine, other = (y, c, z), (y, pc, z)
    own_half = w_ref.at[:, cols(c)]
    push(w_ref.at[:, cols(pc)], w_all.at[mine], sem_w.at[mine], mate)
    both_ways(own_half, w_all.at[mine], sem_w.at[mine])
    push(own_half, w_all.at[mine], sem_w.at[mine], yn_dev)
    x_push(y, 1 - x, 2, xn_dev)
    x_push(yo, 1 - x, 2, xn_dev)
    x_push(y, x, 1, mate)
    x_push(yo, x, 1, mate)
    w_all[mine] = w_ref[:, cols(c)]
    w_arrive(other)
    both_ways(w_all.at[other], w_all.at[other], sem_w.at[other])
    w_push(other, yn_dev)
    kv_all[0, z] = k_ref[...]
    kv_all[1, z] = v_ref[...]
    xs[y, 0] = x_ref[:, width(y, x)]
    xs[yo, 0] = x_ref[:, width(yo, x)]

    step = 16

    @pl.loop(0, rows // step)
    def _(i):
        at = pl.ds(pl.multiple_of(i * step, step), step)
        block = x_ref[at, :].astype(F32)
        factor = lax.rsqrt(jnp.mean(block * block, axis=1, keepdims=True) + EPSILON)
        inv[0, at, :] = jnp.broadcast_to(factor, (step, 128))

    push(inv.at[0], inv.at[1], sem_inv.at[0], mate)

    def sources(k):
        return (
            (z >= k, (z >= k) & (z < 3), (z + 4 - k) % 4, above),
            (z + k <= 3, (z + k <= 3) & (z > 0), (z + k) % 4, below),
        )

    def forward(k):
        for part in range(2):
            for present, onward, chunk, dev in sources(k):
                at = (y, part, chunk)

                @pl.when(present)
                def _():
                    w_arrive(at)

                if k < 3:
                    push_when(onward, w_all.at[at], w_all.at[at], sem_w.at[at], dev)
                push_when(present, w_all.at[at], w_all.at[at], sem_w.at[at], yn_dev)

    def kv_forward(k):
        for part in range(2):
            for present, onward, chunk, dev in sources(k):
                at = (part, chunk)

                @pl.when(present)
                def _():
                    arrive(kv_all.at[at], sem_kv.at[at])

                if k < 3:
                    push_when(onward, kv_all.at[at], kv_all.at[at], sem_kv.at[at], dev)

    def x_arrive(at_y, slot):
        arrive(xs.at[at_y, slot], sem_x.at[at_y, slot])

    def x_relay(at_y):
        x_arrive(at_y, 2)
        push(xs.at[at_y, 2], xs.at[at_y, 3], sem_x.at[at_y, 3], mate)

    def turn(at_y, slot):
        for j in range(depth // 128):
            at = slice(j * 128, (j + 1) * 128)
            xt[at_y, at, slot * rows : (slot + 1) * rows] = xs[at_y, slot, :, at].T

    def w_block(at_y):
        return w_all[at_y].reshape(depth, half)

    def product(at_y, first):
        return jnp.dot(
            xs[at_y, first : first + 2].reshape(2 * rows, depth), w_block(at_y),
            preferred_element_type=F32,
        )

    forward(1)
    both_ways(k_ref, kv_all.at[0, z], sem_kv.at[0, z])
    both_ways(v_ref, kv_all.at[1, z], sem_kv.at[1, z])
    x_arrive(y, 1)
    x_arrive(yo, 1)
    for slot in range(2):

        @pl.loop(0, 2)
        def _(at_y):
            turn(at_y, slot)

    forward(2)
    x_relay(y)
    kv_forward(1)
    forward(3)
    kv_forward(2)
    pred[0] = product(y, 0)
    x_relay(yo)
    x_arrive(y, 3)
    pred[1] = product(y, 2)
    turn(y, 2)
    turn(y, 3)
    x_arrive(yo, 3)
    for r in range(4):
        for part in range(2):
            w_arrive((yo, part, zs[r]))
    p_out[...] = (pred[1] + product(yo, 2)).astype(BF16).reshape(2, rows, half)
    for slot in range(2):
        push(p_out.at[slot], p_in.at[slot], sem_p.at[slot], xn_dev)
    pred[0] += product(yo, 0)

    kv_forward(3)
    ends = []
    total = 0
    for i in range(len_ref.shape[1]):
        total = total + len_ref[0, i]
        ends.append(total)

    def document(position):
        found = jnp.zeros(position.shape, jnp.int32)
        for end in ends:
            found = found + (position >= end).astype(jnp.int32)
        return found

    lanes = lax.broadcasted_iota(jnp.int32, (1, BLK), 1)
    k_pos = jnp.concatenate([asg_ref[0, j] * BLK + lanes for j in range(4)], axis=1)
    q_pos = asg_ref[0, z] * BLK + lax.broadcasted_iota(jnp.int32, (rows, 1), 0)
    allowed = (document(q_pos) == document(k_pos)) & (q_pos >= k_pos)
    k_all = kv_all[0].reshape(4 * rows, HD)
    v_all = kv_all[1].reshape(4 * rows, HD)
    for h in range(HQ):
        scores = lax.dot_general(
            q_ref[:, h * HD : (h + 1) * HD], k_all, (((1,), (1,)), ((), ())),
            preferred_element_type=F32,
        ) * HD ** (-0.5)
        masked = jnp.where(allowed, scores, NEGATIVE)
        top = jnp.max(masked, axis=1, keepdims=True)
        terms = jnp.where(allowed, jnp.exp(masked - top), 0.0)
        totals = jnp.sum(terms, axis=1, keepdims=True)
        mixture = jnp.dot(terms.astype(BF16), v_all, preferred_element_type=F32)
        done = (mixture / totals).astype(BF16)
        att_ref[:, h * HD : (h + 1) * HD] = done
        place = (h % 2) * HD
        att_half[h // 2, :, place : place + HD] = done
    push(att_half.at[pc], att_peer, sem_att.at[0], mate)

    def scale_rows(slot, attended):
        arrive(p_in.at[slot], sem_p.at[slot])
        factor = jnp.concatenate([inv[slot]] * (half // 128), axis=1)
        raw = pred[0, slot * rows : (slot + 1) * rows, :] + p_in[slot].astype(F32)
        gap = raw * factor - attended.astype(F32)
        s_all[slot] = (gap * token_total ** (-0.5) * factor).astype(BF16)
        push(s_all.at[slot], s_all.at[slot + 2], sem_s.at[slot], xn_dev)

    scale_rows(0, att_half[c])
    arrive(att_peer, sem_att.at[0])
    arrive(inv.at[1], sem_inv.at[0])
    scale_rows(1, att_peer[...])
    turn(yo, 2)
    turn(yo, 3)

    def grad(at_y, first):
        return jnp.dot(
            xt[at_y, :, first * rows : (first + 2) * rows],
            s_all[first : first + 2].reshape(2 * rows, half),
            preferred_element_type=F32,
        ).reshape(2, 4, piece, half)

    grad_f[yo] = grad(yo, 0)
    grad_f[y] = grad(y, 0)
    for slot in range(2):
        arrive(s_all.at[slot + 2], sem_s.at[slot])
    s_y[...] = (grad_f[yo] + grad(yo, 2)).astype(BF16)
    order = (3, 2, 1, 0)
    for r in order:
        for part in range(2):
            at = (part, zs[r])
            push(s_y.at[at], r_y.at[at], sem_ry.at[at], yn_dev)
    grad_f[y] += grad(y, 2)

    def column_sum(part, g):
        arrive(r_y.at[part, g], sem_ry.at[part, g])
        return grad_f[y, part, g] + r_y[part, g].astype(F32)

    for r in order[:3]:
        g = zs[r]
        for part in range(2):
            s_z[part, g] = column_sum(part, g).astype(BF16)
        push(s_z.at[c, g], r_z.at[z, c], sem_rz.at[z, c], z_dev[r])
        push(s_z.at[pc, g], r_z.at[z, c], sem_rz.at[z, c], z_mate[r])
    for part in range(2):
        grad_f[y, part, z] = column_sum(part, z)
    s_z[pc, z] = grad_f[y, pc, z].astype(BF16)
    push(s_z.at[pc, z], r_z.at[z, c], sem_rz.at[z, c], mate)
    total = grad_f[y, c, z]
    for r in range(1, 4):
        arrive(r_z.at[zs[r], c], sem_rz.at[zs[r], c])
        total = total + r_z[zs[r], c].astype(F32)
    out_ref[:, cols(c)] = total
    total = jnp.zeros((piece, half), F32)
    for r in (3, 2, 1, 0):
        arrive(r_z.at[zs[r], pc], sem_rz.at[zs[r], pc])
        total = total + r_z[zs[r], pc].astype(F32)
    out_ref[:, cols(pc)] = total
    for copy in sent:
        copy.wait_send()
    for present, copy in sent_when:
        pl.when(present)(copy.wait_send)


def local_fused(student_in, weight, queries, keys, values, lengths, assignment):
    rows, width = student_in.shape
    piece, features = weight.shape
    half = features // 2
    depth = width // 4
    token_total = rows * lax.axis_size("dp") * lax.axis_size("seq")
    vmem = pl.BlockSpec(memory_space=pltpu.VMEM)
    smem = pl.BlockSpec(memory_space=pltpu.SMEM)
    dma = pltpu.SemaphoreType.DMA
    quarter = (2, 4, piece, half)
    return pl.pallas_call(
        functools.partial(fused_kernel, token_total),
        out_shape=(
            jax.ShapeDtypeStruct((rows, features), BF16),
            jax.ShapeDtypeStruct((piece, features), F32),
        ),
        in_specs=[vmem] * 5 + [smem] * 2,
        out_specs=(vmem, vmem),
        scratch_shapes=[
            pltpu.VMEM((2, 4, rows, depth), BF16),
            pltpu.VMEM((2, depth, 4 * rows), BF16),
            pltpu.VMEM((2,) + quarter, BF16),
            pltpu.VMEM((2, 4, rows, HD), BF16),
            pltpu.VMEM((2, rows, 128), F32),
            pltpu.VMEM((2, 2 * rows, half), F32),
            pltpu.VMEM((2, rows, half), BF16),
            pltpu.VMEM((2, rows, half), BF16),
            pltpu.VMEM((4, rows, half), BF16),
            pltpu.VMEM((2, rows, half), BF16),
            pltpu.VMEM((rows, half), BF16),
            pltpu.VMEM((2,) + quarter, F32),
            pltpu.VMEM(quarter, BF16),
            pltpu.VMEM(quarter, BF16),
            pltpu.VMEM(quarter, BF16),
            pltpu.VMEM((4, 2, piece, half), BF16),
            dma((64,)),
            dma((64,)),
            dma((2, 2, 4)),
            dma((2, 4)),
            dma((2, 4)),
            dma((1,)),
            dma((1,)),
            dma((2,)),
            dma((2,)),
            dma((2, 4)),
            dma((4, 2)),
        ],
        compiler_params=pltpu.CompilerParams(collective_id=0, has_side_effects=True),
        name="distill",
    )(student_in, weight, queries, keys, values, lengths, assignment)


def fits(student_in, weight, queries, keys, values, lengths, assignment):
    rows, width = student_in.shape
    piece, features = weight.shape
    return (
        lax.axis_size("dp") == 8
        and lax.axis_size("seq") == 4
        and rows == BLK
        and assignment.shape[1] == 4
        and piece % 16 == 0
        and width == 32 * piece
        and width % 512 == 0
        and features == HQ * HD
        and keys.shape[1] == HD
    )


def dispatch(*arrays):
    return local_fused(*arrays) if fits(*arrays) else local(*arrays)


def solution(mesh):
    placed = (
        P(("dp", "seq"), None),
        P(("dp", "seq"), None),
        P(("dp", "seq"), None),
        P(("dp", "seq"), None),
        P(("dp", "seq"), None),
        P("dp", None),
        P("dp", None),
    )
    return jax.shard_map(
        dispatch,
        mesh=mesh,
        in_specs=placed,
        out_specs=(P(("dp", "seq"), None), P(("dp", "seq"), None)),
        check_vma=False,
    )
```
